32 devices in a mesh: heads: 2 (over x), seq: 16 (over z, y, core).
Axes of the slice: x: 2, y: 2, z: 4, core: 2. Of those that a mesh axis runs over, the one named last changes fastest.
Arguments:
- query_nope: bfloat16 [1, 4, 128, 128], P(None, None, 'heads'), may hold values from -6 to 6
- query_rope: bfloat16 [1, 4, 128, 64], P(None, None, 'heads'), may hold values from -8 to 8
- latent_cache: bfloat16 [1, 8192, 512], P(None, 'seq'), may hold values from -6 to 6
- rope_keys: bfloat16 [1, 64, 8192], P(None, None, 'seq'), may hold values from -8 to 8
- lengths: int32 [1], replicated, may hold values from 2 to 8189, as said below
- key_quant: bfloat16 [128, 512, 128], P('heads', 'seq'), may hold values from -127 to 127, as said below
- key_scale: float32 [128, 4], P('heads'), may hold values from 0.0006 to 0.0024
- value_quant: bfloat16 [128, 512, 128], P('heads', 'seq'), may hold values from -127 to 127, as said below
- value_scale: float32 [128, 4], P('heads'), may hold values from 0.0003 to 0.0012
- out_weight: bfloat16 [16384, 7168], P('heads', 'seq'), may hold values from -0.375 to 0.375
Outputs:
- attn_out: bfloat16 [1, 4, 7168], P(None, None, 'seq')
The draws below stay inside these ranges and needn't reach their ends.
Inputs may be any that keep to these rules, and one draw needn't show every extreme that they name: `key_quant`: whole numbers. `value_quant`: whole numbers. `lengths`: one sequence has the largest allowed length, so that its last draft token sees all 8192 positions.
All inputs are finite; a program needn't handle non-finite values.
Results may differ from the reference program's by a relative error of at most 0.019.
Values may be sent and summed in bfloat16 or wider, within the bound.
A program may use at most 64 MiB of HBM per device.

```python
import math
import jax
import jax.numpy as jnp
from jax import lax

H = 128
C = 512
R = 64
NOPE = 128
V = 128
D = 7168
QB = 128
B = 1
QT = 4
CTX_DEV = 512
CONTEXT = 8192
N_SEQ = 16


def rope_pair(key):
    base_key = jax.random.fold_in(key, 911)
    key_query, key_cache = jax.random.split(base_key, 2)
    queries = jnp.clip(jax.random.normal(key_query, (B, QT, H, R), jnp.float32), -8.0, 8.0)
    keys_out = jnp.clip(jax.random.normal(key_cache, (B, R, CONTEXT), jnp.float32), -8.0, 8.0)
    return (queries, keys_out)


def draw_query_rope(key, part):
    return rope_pair(key)[0].astype(jnp.bfloat16)


def draw_rope_keys(key, part):
    return rope_pair(key)[1].astype(jnp.bfloat16)


def draw_lengths(key, part):
    values = jax.random.randint(jax.random.fold_in(key, 3), (B,), 2, CONTEXT - QT + 2)
    longest = jax.random.randint(jax.random.fold_in(key, 5), (), 0, B)
    return jnp.where(jnp.arange(B) == longest, CONTEXT - QT + 1, values).astype(jnp.int32)


def draw_key_quant(key, part):
    values = jax.random.randint(jax.random.fold_in(key, 7), (H, C, NOPE), -127, 128)
    return values.astype(jnp.float32).astype(jnp.bfloat16)


def draw_value_quant(key, part):
    values = jax.random.randint(jax.random.fold_in(key, 11), (H, C, V), -127, 128)
    return values.astype(jnp.float32).astype(jnp.bfloat16)


def steps_of(own_key, dims, cuts, least, high):
    factor_of = 1.0
    for dim, shards_of in cuts:
        draws = jax.random.uniform(jax.random.fold_in(jax.random.fold_in(own_key, 6), dim), (shards_of,), jnp.float32, least / len(cuts), high / len(cuts))
        factor_of = factor_of * jnp.repeat(jnp.exp(draws), dims[dim] // shards_of).reshape((-1,) + (1,) * (len(dims) - 1 - dim))
    return factor_of


def normal_values(own_key, shape, spread, limit, cuts=(), held_as=jnp.bfloat16):
    drawn = spread * jax.random.normal(own_key, shape, jnp.float32)
    if cuts:
        drawn = drawn * steps_of(own_key, shape, cuts, -0.22, 0.18)
    return jnp.clip(drawn, -limit, limit).astype(held_as)


def setup_inputs(seed: int = 0) -> dict:
    seeds = jax.random.split(jax.random.key(seed), 11)
    return {
        "query_nope": normal_values(seeds[0], (B, QT, H, NOPE), 1.0, 6.0, ((2, 2),)),
        "query_rope": draw_query_rope(jax.random.fold_in(seeds[10], 71), 0),
        "latent_cache": normal_values(seeds[2], (B, CONTEXT, C), 1.0, 6.0, ((1, 16),)),
        "rope_keys": draw_rope_keys(jax.random.fold_in(seeds[10], 71), 0),
        "lengths": draw_lengths(jax.random.fold_in(seeds[10], 71), 0),
        "key_quant": draw_key_quant(jax.random.fold_in(seeds[10], 71), 0),
        "key_scale": jnp.clip(jnp.exp(math.log(0.0024) - 1.3862944 * jax.random.uniform(seeds[6], (H, C // QB), jnp.float32) ** steps_of(seeds[6], (H, C // QB), ((0, 2),), -0.2, 0.2)), 0.0006, 0.0024),
        "value_quant": draw_value_quant(jax.random.fold_in(seeds[10], 71), 0),
        "value_scale": jnp.clip(jnp.exp(math.log(0.0012) - 1.3862944 * jax.random.uniform(seeds[8], (H, C // QB), jnp.float32) ** steps_of(seeds[8], (H, C // QB), ((0, 2),), -0.2, 0.2)), 0.0003, 0.0012),
        "out_weight": normal_values(seeds[9], (H * V, D), (H * V // 64) ** -0.5, 0.375, ((0, 2), (1, 16))),
    }


neg_large = -1.0e30


def expand_scales(block_scale, offset, count):
    row_ids = (offset + jnp.arange(count, dtype=jnp.int32)) // QB
    onehot = (row_ids[:, None] == jnp.arange(block_scale.shape[1], dtype=jnp.int32)[None, :]).astype(block_scale.dtype)
    return jnp.sum(block_scale[:, None, :] * onehot[None, :, :], axis=2)


def dequantize(quantized, block_scale, offset):
    factors = expand_scales(block_scale, offset, quantized.shape[1])
    return (quantized.astype(jnp.float32) * factors[:, :, None]).astype(jnp.bfloat16)


def combine(earlier, later):
    max_a, sum_a, out_a = earlier
    max_b, sum_b, out_b = later
    joint = jnp.maximum(max_a, max_b)
    fac_a = jnp.exp(max_a - joint)
    fac_b = jnp.exp(max_b - joint)
    return joint, sum_a * fac_a + sum_b * fac_b, out_a * fac_a[..., None] + out_b * fac_b[..., None]


def reference(query_nope, query_rope, latent_cache, rope_keys, lengths, key_quant, key_scale, value_quant, value_scale, out_weight):
    key_weight = dequantize(key_quant, key_scale, 0)
    value_weight = dequantize(value_quant, value_scale, 0)
    query_latent = jnp.einsum("btkn,kcn->btkc", query_nope.astype(jnp.float32), key_weight.astype(jnp.float32)).astype(jnp.bfloat16)
    factor = (NOPE + R) ** -0.5
    horizon = lengths[:, None] + jnp.arange(QT, dtype=jnp.int32)[None, :]
    lat_f = query_latent.astype(jnp.float32)
    rope_f = query_rope.astype(jnp.float32)

    def one_block(state_acc, block_idx):
        offset = (block_idx * CTX_DEV).astype(jnp.int32)
        cache_blk = lax.dynamic_slice_in_dim(latent_cache, offset, CTX_DEV, 1).astype(jnp.float32)
        rope_blk = lax.dynamic_slice_in_dim(rope_keys, offset, CTX_DEV, 2).astype(jnp.float32)
        scores = (jnp.einsum("btkc,bsc->btks", lat_f, cache_blk) + jnp.einsum("btkr,brs->btks", rope_f, rope_blk)) * factor
        position = offset + jnp.arange(CTX_DEV, dtype=jnp.int32)
        visible = (position[None, None, :] < horizon[:, :, None])[:, :, None, :]
        block_max = jnp.max(jnp.where(visible, scores, neg_large), axis=3)
        probs = jnp.where(visible, jnp.exp(scores - block_max[..., None]), 0.0)
        block_sum = jnp.sum(probs, axis=3)
        probs_bf = probs.astype(jnp.bfloat16)
        block_out = jnp.einsum("btks,bsc->btkc", probs_bf.astype(jnp.float32), cache_blk)
        return combine(state_acc, (block_max, block_sum, block_out)), None

    start_state = (jnp.full((B, QT, H), neg_large, jnp.float32), jnp.zeros((B, QT, H), jnp.float32), jnp.zeros((B, QT, H, C), jnp.float32))
    final_state, _ = lax.scan(one_block, start_state, jnp.arange(N_SEQ, dtype=jnp.int32))
    out_latent = (final_state[2] / final_state[1][..., None]).astype(jnp.bfloat16)
    head_output = jnp.einsum("btkc,kcv->btkv", out_latent.astype(jnp.float32), value_weight.astype(jnp.float32)).astype(jnp.bfloat16)
    summed = jnp.dot(head_output.reshape(B * QT, H * V), out_weight, preferred_element_type=jnp.float32)
    return summed.astype(jnp.bfloat16).reshape(B, QT, D)
```

```python
import functools

import jax
import jax.numpy as jnp
from jax import lax
from jax.experimental import pallas as pl
from jax.experimental.pallas import tpu as pltpu
from jax.sharding import PartitionSpec as P

QB = 128
MESH = pl.DeviceIdType.MESH
neg_large = -1e30
F32 = jnp.float32
BF16 = jnp.bfloat16


def scale_row(scale_ref, block, rows, heads):
    scales = scale_ref[...]
    column = jnp.sum(
        jnp.where(lax.broadcasted_iota(jnp.int32, scales.shape, 1) == block, scales, 0.0),
        axis=1,
        keepdims=True,
    )
    lane_head = lax.broadcasted_iota(jnp.int32, (heads, rows), 1) % heads
    own_head = lax.broadcasted_iota(jnp.int32, (heads, rows), 0)
    return jnp.sum(jnp.where(lane_head == own_head, column, 0.0), axis=0, keepdims=True)


def kernel(
    n,
    groups,
    heads,
    drafts,
    q_hbm,
    qr_hbm,
    cache_hbm,
    rope_hbm,
    len_ref,
    kq_hbm,
    ks_ref,
    vq_hbm,
    vs_ref,
    w_hbm,
    out_ref,
    q,
    qr,
    cache,
    rope,
    kq,
    vq,
    w,
    cache_t,
    vq_t,
    base,
    lat_all,
    stats,
    out_send,
    out_recv,
    part_send,
    part_recv,
    share_all,
    flat,
    heads_out,
    final,
    in_sem,
    lat_send,
    lat_recv,
    st_send,
    st_recv,
    o_send,
    o_recv,
    p_send,
    p_recv,
    s_send,
    s_recv,
    f_send,
    f_recv,
):
    me = lax.axis_index("seq")
    group = lax.axis_index("heads")
    rows = q.shape[0]
    cols = lat_all.shape[1]
    width = vq.shape[1]
    positions = cache.shape[0]
    factor = (q.shape[1] + qr.shape[1]) ** (-0.5)

    loads = []
    for i, (src, dst) in enumerate(
        ((kq_hbm, kq), (q_hbm, q), (qr_hbm, qr), (rope_hbm, rope), (cache_hbm, cache), (vq_hbm, vq), (w_hbm, w))
    ):
        copy = pltpu.make_async_copy(src, dst, in_sem.at[i])
        copy.start()
        loads.append(copy)
    kq_load, q_load, qr_load, rope_load, cache_load, vq_load, w_load = loads

    barrier = pltpu.get_barrier_semaphore()

    def greet_seq(j, c):
        pl.semaphore_signal(barrier, inc=1, device_id=(group, lax.rem(me + j, n)), device_id_type=MESH)
        return c

    def greet_heads(j, c):
        pl.semaphore_signal(barrier, inc=1, device_id=(lax.rem(group + j, groups), me), device_id_type=MESH)
        return c

    lax.fori_loop(1, n, greet_seq, 0)
    lax.fori_loop(1, groups, greet_heads, 0)

    def spread(src_of, dst, send, recv):
        def make(j):
            peer = lax.rem(me + j, n)
            return pltpu.make_async_remote_copy(
                src_ref=src_of(peer),
                dst_ref=dst.at[me],
                send_sem=send.at[peer],
                recv_sem=recv.at[me],
                device_id=(group, peer),
                device_id_type=MESH,
            )

        def go(j, c):
            make(j).start()
            return c

        lax.fori_loop(1, n, go, 0)

    def arrive(src_of, dst, send, recv):
        def wait(j, c):
            peer = lax.rem(me + j, n)
            pltpu.make_async_remote_copy(
                src_ref=src_of(peer),
                dst_ref=dst.at[peer],
                send_sem=send.at[peer],
                recv_sem=recv.at[peer],
                device_id=(group, peer),
                device_id_type=MESH,
            ).wait_recv()
            return c

        lax.fori_loop(1, n, wait, 0)

    def drain(src_of, dst, send, recv):
        def wait(j, c):
            peer = lax.rem(me + j, n)
            pltpu.make_async_remote_copy(
                src_ref=src_of(peer),
                dst_ref=dst.at[me],
                send_sem=send.at[peer],
                recv_sem=recv.at[me],
                device_id=(group, peer),
                device_id_type=MESH,
            ).wait_send()
            return c

        lax.fori_loop(1, n, wait, 0)

    block = (me * cols) // QB
    lane_head = lax.broadcasted_iota(jnp.int32, (1, rows), 1) % heads
    key_row = scale_row(ks_ref, block, rows, heads)
    value_row = scale_row(vs_ref, block, rows, heads)

    kq_load.wait()
    q_load.wait()
    every = lax.dot_general(kq[...], q[...], (((1,), (1,)), ((), ())), preferred_element_type=F32)
    every = every.reshape(heads, cols, rows)
    own = lax.broadcasted_iota(jnp.int32, (heads, 1, rows), 0) == lane_head[None]
    piece = jnp.sum(jnp.where(own, every, 0.0), axis=0) * key_row
    lat_all[me] = piece.astype(BF16)

    pl.semaphore_wait(barrier, n - 1 + groups - 1)
    lat = (lambda peer: lat_all.at[me], lat_all, lat_send, lat_recv)
    spread(*lat)

    qr_load.wait()
    rope_load.wait()
    base[...] = lax.dot_general(
        rope[...].T, qr[...], (((1,), (1,)), ((), ())), preferred_element_type=F32
    )
    cache_load.wait()
    cache_t[...] = cache[...].T
    vq_load.wait()
    vq_t[...] = vq[...].T
    position = me * positions + lax.broadcasted_iota(jnp.int32, (positions, rows), 0)
    horizon = len_ref[0] + lax.broadcasted_iota(jnp.int32, (positions, rows), 1) // heads
    visible = position < horizon

    arrive(*lat)
    query_latent = lat_all[...].reshape(n * cols, rows)
    scores = (jnp.dot(cache[...], query_latent, preferred_element_type=F32) + base[...]) * factor
    block_max = jnp.max(jnp.where(visible, scores, neg_large), axis=0, keepdims=True)
    probs = jnp.where(visible, jnp.exp(scores - block_max), 0.0)
    block_sum = jnp.sum(probs, axis=0, keepdims=True)
    stats[me, 0:1, :] = block_max
    stats[me, 1:2, :] = block_sum
    st = (lambda peer: stats.at[me], stats, st_send, st_recv)
    spread(*st)
    block_out = jnp.dot(cache_t[...], probs.astype(BF16), preferred_element_type=F32)
    out_send[...] = block_out.astype(BF16).reshape(n, cols, rows)
    o = (lambda peer: out_send.at[peer], out_recv, o_send, o_recv)
    spread(*o)
    out_recv[me] = out_send[me]

    arrive(*st)
    all_max = stats[:, 0:1, :]
    top = jnp.max(all_max, axis=0, keepdims=True)
    weight = jnp.exp(all_max - top)
    total = jnp.sum(weight * stats[:, 1:2, :], axis=0)
    arrive(*o)
    merged = jnp.sum(out_recv[...].astype(F32) * weight, axis=0) / total
    latent = jnp.where(own, merged[None], 0.0).astype(BF16).reshape(heads * cols, rows)
    partial = jnp.dot(vq_t[...], latent, preferred_element_type=F32) * value_row
    step = width // n
    for d in range(n):
        part_send[d] = partial[d * step : (d + 1) * step].astype(part_send.dtype)
    p = (lambda peer: part_send.at[peer], part_recv, p_send, p_recv)
    spread(*p)
    part_recv[me] = part_send[me]
    arrive(*p)
    share_all[me] = jnp.sum(part_recv[...].astype(F32), axis=0).astype(BF16)
    s = (lambda peer: share_all.at[me], share_all, s_send, s_recv)
    spread(*s)
    arrive(*s)
    head_t = jnp.concatenate([share_all[d].astype(F32) for d in range(n)], axis=0)
    heads_out[...] = head_t.T.reshape(drafts, heads, width)
    for k in range(heads):
        flat[:, k * width : (k + 1) * width] = heads_out[:, k, :].astype(BF16)
    w_load.wait()
    final[group] = jnp.dot(flat[...], w[...], preferred_element_type=F32)

    def pair(j, at):
        peer = lax.rem(group + j, groups)
        return pltpu.make_async_remote_copy(
            src_ref=final.at[group],
            dst_ref=final.at[group if at else peer],
            send_sem=f_send.at[peer],
            recv_sem=f_recv.at[group if at else peer],
            device_id=(peer, me),
            device_id_type=MESH,
        )

    for j in range(1, groups):
        pair(j, True).start()
    for j in range(1, groups):
        pair(j, False).wait_recv()
    out_ref[...] = jnp.sum(final[...], axis=0).astype(BF16)
    for each in (lat, st, o, p, s):
        drain(*each)
    for j in range(1, groups):
        pair(j, True).wait_send()


def solution(mesh):
    n = mesh.shape["seq"]
    groups = mesh.shape["heads"]

    def per_device(
        query_nope,
        query_rope,
        latent_cache,
        rope_keys,
        lengths,
        key_quant,
        key_scale,
        value_quant,
        value_scale,
        out_weight,
    ):
        batch, drafts, heads, nope = query_nope.shape
        rows = batch * drafts * heads
        rope = query_rope.shape[-1]
        positions, latent = latent_cache.shape[1:]
        cols = key_quant.shape[1]
        width = value_quant.shape[2]
        model = out_weight.shape[1]
        hbm = pl.BlockSpec(memory_space=pltpu.HBM)
        vmem = pl.BlockSpec(memory_space=pltpu.VMEM)
        smem = pl.BlockSpec(memory_space=pltpu.SMEM)
        dma = pltpu.SemaphoreType.DMA
        result = pl.pallas_call(
            functools.partial(kernel, n, groups, heads, drafts),
            out_shape=jax.ShapeDtypeStruct((drafts, model), BF16),
            in_specs=[hbm, hbm, hbm, hbm, smem, hbm, vmem, hbm, vmem, hbm],
            out_specs=vmem,
            scratch_shapes=[
                pltpu.VMEM((rows, nope), BF16),
                pltpu.VMEM((rows, rope), BF16),
                pltpu.VMEM((positions, latent), BF16),
                pltpu.VMEM((rope, positions), BF16),
                pltpu.VMEM((heads * cols, nope), BF16),
                pltpu.VMEM((heads * cols, width), BF16),
                pltpu.VMEM(out_weight.shape, BF16),
                pltpu.VMEM((latent, positions), BF16),
                pltpu.VMEM((width, heads * cols), BF16),
                pltpu.VMEM((positions, rows), F32),
                pltpu.VMEM((n, cols, rows), BF16),
                pltpu.VMEM((n, 2, rows), F32),
                pltpu.VMEM((n, cols, rows), BF16),
                pltpu.VMEM((n, cols, rows), BF16),
                pltpu.VMEM((n, width // n, rows), BF16),
                pltpu.VMEM((n, width // n, rows), BF16),
                pltpu.VMEM((n, width // n, rows), BF16),
                pltpu.VMEM((drafts, heads * width), BF16),
                pltpu.VMEM((drafts, heads, width), F32),
                pltpu.VMEM((groups, drafts, model), F32),
                dma((7,)),
            ]
            + [dma((n,))] * 10
            + [dma((groups,))] * 2,
            compiler_params=pltpu.CompilerParams(
                collective_id=0, has_side_effects=True, vmem_limit_bytes=48 * 1024 * 1024
            ),
        )(
            query_nope.reshape(rows, nope),
            query_rope.reshape(rows, rope),
            latent_cache.reshape(positions, latent),
            rope_keys.reshape(rope, positions),
            lengths,
            key_quant.reshape(heads * cols, nope),
            key_scale,
            value_quant.reshape(heads * cols, width),
            value_scale,
            out_weight,
        )
        return result.reshape(batch, drafts, model)

    in_specs = (
        P(None, None, "heads", None),
        P(None, None, "heads", None),
        P(None, "seq", None),
        P(None, None, "seq"),
        P(),
        P("heads", "seq", None),
        P("heads", None),
        P("heads", "seq", None),
        P("heads", None),
        P("heads", "seq"),
    )
    return jax.shard_map(
        per_device, mesh=mesh, in_specs=in_specs, out_specs=P(None, None, "seq"), check_vma=False
    )
```

```python
import functools

import jax
import jax.numpy as jnp
from jax import lax
from jax.experimental import pallas as pl
from jax.experimental.pallas import tpu as pltpu
from jax.sharding import PartitionSpec as P

QB = 128
MESH = pl.DeviceIdType.MESH
neg_large = -1e30
F32 = jnp.float32
BF16 = jnp.bfloat16


def scale_row(scale_ref, block, rows, heads):
    scales = scale_ref[...]
    line = jnp.sum(
        jnp.where(lax.broadcasted_iota(jnp.int32, scales.shape, 0) == block, scales, 0.0),
        axis=0,
        keepdims=True,
    )
    square = (heads, heads)
    diagonal = lax.broadcasted_iota(jnp.int32, square, 0) == lax.broadcasted_iota(jnp.int32, square, 1)
    column = jnp.sum(jnp.where(diagonal, line, 0.0), axis=1, keepdims=True)
    lane_head = lax.broadcasted_iota(jnp.int32, (heads, rows), 1) % heads
    own_head = lax.broadcasted_iota(jnp.int32, (heads, rows), 0)
    return jnp.sum(jnp.where(lane_head == own_head, column, 0.0), axis=0, keepdims=True)


def kernel(
    n,
    groups,
    heads,
    drafts,
    q_hbm,
    qr_hbm,
    cache_hbm,
    rope_hbm,
    len_ref,
    kq_hbm,
    ks_ref,
    vq_hbm,
    vs_ref,
    w_hbm,
    out_ref,
    q,
    qr,
    cache,
    rope,
    kq,
    vq,
    w,
    cache_t,
    vq_t,
    base,
    lat_all,
    stats,
    out_send,
    out_recv,
    part_send,
    part_recv,
    share_all,
    flat,
    heads_out,
    final,
    in_sem,
    lat_send,
    lat_recv,
    st_send,
    st_recv,
    o_send,
    o_recv,
    p_send,
    p_recv,
    s_send,
    s_recv,
    f_send,
    f_recv,
):
    me = lax.axis_index("seq")
    group = lax.axis_index("heads")
    rows = q.shape[0]
    cols = lat_all.shape[1]
    width = vq.shape[1]
    positions = cache.shape[0]
    factor = (q.shape[1] + qr.shape[1]) ** (-0.5)

    loads = []
    for i, (src, dst) in enumerate(
        ((kq_hbm, kq), (q_hbm, q), (qr_hbm, qr), (rope_hbm, rope), (cache_hbm, cache), (vq_hbm, vq), (w_hbm, w))
    ):
        copy = pltpu.make_async_copy(src, dst, in_sem.at[i])
        copy.start()
        loads.append(copy)
    kq_load, q_load, qr_load, rope_load, cache_load, vq_load, w_load = loads

    barrier = pltpu.get_barrier_semaphore()

    def greet_seq(j, c):
        pl.semaphore_signal(barrier, inc=1, device_id=(group, lax.rem(me + j, n)), device_id_type=MESH)
        return c

    def greet_heads(j, c):
        pl.semaphore_signal(barrier, inc=1, device_id=(lax.rem(group + j, groups), me), device_id_type=MESH)
        return c

    lax.fori_loop(1, n, greet_seq, 0)
    lax.fori_loop(1, groups, greet_heads, 0)

    def spread(src_of, dst, send, recv):
        def make(j):
            peer = lax.rem(me + j, n)
            return pltpu.make_async_remote_copy(
                src_ref=src_of(peer),
                dst_ref=dst.at[me],
                send_sem=send.at[peer],
                recv_sem=recv.at[me],
                device_id=(group, peer),
                device_id_type=MESH,
            )

        def go(j, c):
            make(j).start()
            return c

        lax.fori_loop(1, n, go, 0)

    def arrive(src_of, dst, send, recv):
        def wait(j, c):
            peer = lax.rem(me + j, n)
            pltpu.make_async_remote_copy(
                src_ref=src_of(peer),
                dst_ref=dst.at[peer],
                send_sem=send.at[peer],
                recv_sem=recv.at[peer],
                device_id=(group, peer),
                device_id_type=MESH,
            ).wait_recv()
            return c

        lax.fori_loop(1, n, wait, 0)

    def drain(src_of, dst, send, recv):
        def wait(j, c):
            peer = lax.rem(me + j, n)
            pltpu.make_async_remote_copy(
                src_ref=src_of(peer),
                dst_ref=dst.at[me],
                send_sem=send.at[peer],
                recv_sem=recv.at[me],
                device_id=(group, peer),
                device_id_type=MESH,
            ).wait_send()
            return c

        lax.fori_loop(1, n, wait, 0)

    block = (me * cols) // QB
    lane_head = lax.broadcasted_iota(jnp.int32, (1, rows), 1) % heads
    key_row = scale_row(ks_ref, block, rows, heads)
    value_row = scale_row(vs_ref, block, rows, heads)

    kq_load.wait()
    q_load.wait()
    every = lax.dot_general(kq[...], q[...], (((1,), (1,)), ((), ())), preferred_element_type=F32)
    every = every.reshape(heads, cols, rows)
    own = lax.broadcasted_iota(jnp.int32, (heads, 1, rows), 0) == lane_head[None]
    piece = jnp.sum(jnp.where(own, every, 0.0), axis=0) * key_row
    lat_all[me] = piece.astype(BF16)

    pl.semaphore_wait(barrier, n - 1 + groups - 1)
    lat = (lambda peer: lat_all.at[me], lat_all, lat_send, lat_recv)
    spread(*lat)

    qr_load.wait()
    rope_load.wait()
    base[...] = lax.dot_general(
        rope[...].T, qr[...], (((1,), (1,)), ((), ())), preferred_element_type=F32
    )
    cache_load.wait()
    cache_t[...] = cache[...].T
    vq_load.wait()
    vq_t[...] = vq[...].T
    position = me * positions + lax.broadcasted_iota(jnp.int32, (positions, rows), 0)
    horizon = len_ref[0] + lax.broadcasted_iota(jnp.int32, (positions, rows), 1) // heads
    visible = position < horizon

    arrive(*lat)
    query_latent = lat_all[...].reshape(n * cols, rows)
    scores = (jnp.dot(cache[...], query_latent, preferred_element_type=F32) + base[...]) * factor
    block_max = jnp.max(jnp.where(visible, scores, neg_large), axis=0, keepdims=True)
    probs = jnp.where(visible, jnp.exp(scores - block_max), 0.0)
    block_sum = jnp.sum(probs, axis=0, keepdims=True)
    stats[me, 0:1, :] = block_max
    stats[me, 1:2, :] = block_sum
    st = (lambda peer: stats.at[me], stats, st_send, st_recv)
    spread(*st)
    block_out = jnp.dot(cache_t[...], probs.astype(BF16), preferred_element_type=F32)
    out_send[...] = block_out.astype(BF16).reshape(n, cols, rows)
    o = (lambda peer: out_send.at[peer], out_recv, o_send, o_recv)
    spread(*o)
    out_recv[me] = out_send[me]

    arrive(*st)
    all_max = stats[:, 0:1, :]
    top = jnp.max(all_max, axis=0, keepdims=True)
    weight = jnp.exp(all_max - top)
    total = jnp.sum(weight * stats[:, 1:2, :], axis=0)
    arrive(*o)
    merged = jnp.sum(out_recv[...].astype(F32) * weight, axis=0) / total
    latent = jnp.where(own, merged[None], 0.0).astype(BF16).reshape(heads * cols, rows)
    partial = jnp.dot(vq_t[...], latent, preferred_element_type=F32) * value_row
    step = width // n
    for d in range(n):
        part_send[d] = partial[d * step : (d + 1) * step].astype(part_send.dtype)
    p = (lambda peer: part_send.at[peer], part_recv, p_send, p_recv)
    spread(*p)
    part_recv[me] = part_send[me]
    arrive(*p)
    share_all[me] = jnp.sum(part_recv[...].astype(F32), axis=0).astype(BF16)
    s = (lambda peer: share_all.at[me], share_all, s_send, s_recv)
    spread(*s)
    arrive(*s)
    head_t = jnp.concatenate([share_all[d].astype(F32) for d in range(n)], axis=0)
    heads_out[...] = head_t.T.reshape(drafts, heads, width)
    for k in range(heads):
        flat[:, k * width : (k + 1) * width] = heads_out[:, k, :].astype(BF16)
    w_load.wait()
    final[group] = lax.dot_general(
        flat[...], w[...], (((1,), (1,)), ((), ())), preferred_element_type=F32
    )

    def pair(j, at):
        peer = lax.rem(group + j, groups)
        return pltpu.make_async_remote_copy(
            src_ref=final.at[group],
            dst_ref=final.at[group if at else peer],
            send_sem=f_send.at[peer],
            recv_sem=f_recv.at[group if at else peer],
            device_id=(peer, me),
            device_id_type=MESH,
        )

    for j in range(1, groups):
        pair(j, True).start()
    for j in range(1, groups):
        pair(j, False).wait_recv()
    out_ref[...] = jnp.sum(final[...], axis=0).astype(BF16)
    for each in (lat, st, o, p, s):
        drain(*each)
    for j in range(1, groups):
        pair(j, True).wait_send()


def solution(mesh):
    n = mesh.shape["seq"]
    groups = mesh.shape["heads"]

    def per_device(
        query_nope,
        query_rope,
        latent_cache,
        rope_keys,
        lengths,
        key_quant,
        key_scale,
        value_quant,
        value_scale,
        out_weight,
    ):
        batch, drafts, heads, nope = query_nope.shape
        rows = batch * drafts * heads
        rope = query_rope.shape[-1]
        positions, latent = latent_cache.shape[1:]
        cols = key_quant.shape[1]
        width = value_quant.shape[2]
        model = out_weight.shape[1]
        hbm = pl.BlockSpec(memory_space=pltpu.HBM)
        vmem = pl.BlockSpec(memory_space=pltpu.VMEM)
        smem = pl.BlockSpec(memory_space=pltpu.SMEM)
        dma = pltpu.SemaphoreType.DMA
        result = pl.pallas_call(
            functools.partial(kernel, n, groups, heads, drafts),
            out_shape=jax.ShapeDtypeStruct((drafts, model), BF16),
            in_specs=[hbm, hbm, hbm, hbm, smem, hbm, vmem, hbm, vmem, hbm],
            out_specs=vmem,
            scratch_shapes=[
                pltpu.VMEM((rows, nope), BF16),
                pltpu.VMEM((rows, rope), BF16),
                pltpu.VMEM((positions, latent), BF16),
                pltpu.VMEM((rope, positions), BF16),
                pltpu.VMEM((heads * cols, nope), BF16),
                pltpu.VMEM((heads * cols, width), BF16),
                pltpu.VMEM(out_weight.shape[::-1], BF16),
                pltpu.VMEM((latent, positions), BF16),
                pltpu.VMEM((width, heads * cols), BF16),
                pltpu.VMEM((positions, rows), F32),
                pltpu.VMEM((n, cols, rows), BF16),
                pltpu.VMEM((n, 2, rows), F32),
                pltpu.VMEM((n, cols, rows), BF16),
                pltpu.VMEM((n, cols, rows), BF16),
                pltpu.VMEM((n, width // n, rows), BF16),
                pltpu.VMEM((n, width // n, rows), BF16),
                pltpu.VMEM((n, width // n, rows), BF16),
                pltpu.VMEM((drafts, heads * width), BF16),
                pltpu.VMEM((drafts, heads, width), F32),
                pltpu.VMEM((groups, drafts, model), F32),
                dma((7,)),
            ]
            + [dma((n,))] * 10
            + [dma((groups,))] * 2,
            compiler_params=pltpu.CompilerParams(
                collective_id=0, has_side_effects=True, vmem_limit_bytes=63 * 1024 * 1024
            ),
        )(
            query_nope.reshape(rows, nope),
            query_rope.reshape(rows, rope),
            latent_cache.reshape(positions, latent),
            rope_keys.reshape(rope, positions),
            lengths,
            key_quant.reshape(heads * cols, nope),
            key_scale.T,
            value_quant.reshape(heads * cols, width),
            value_scale.T,
            out_weight.T,
        )
        return result.reshape(batch, drafts, model)

    in_specs = (
        P(None, None, "heads", None),
        P(None, None, "heads", None),
        P(None, "seq", None),
        P(None, None, "seq"),
        P(),
        P("heads", "seq", None),
        P("heads", None),
        P("heads", "seq", None),
        P("heads", None),
        P("heads", "seq"),
    )
    return jax.shard_map(
        per_device, mesh=mesh, in_specs=in_specs, out_specs=P(None, None, "seq"), check_vma=False
    )
```

```python
import functools

import jax
import jax.numpy as jnp
from jax import lax
from jax.experimental import pallas as pl
from jax.experimental.pallas import tpu as pltpu
from jax.sharding import PartitionSpec as P

QB = 128
MESH = pl.DeviceIdType.MESH
neg_large = -1e30
F32 = jnp.float32
BF16 = jnp.bfloat16


def scale_row(scale_ref, block, rows, heads):
    scales = scale_ref[...]
    line = jnp.sum(
        jnp.where(lax.broadcasted_iota(jnp.int32, scales.shape, 0) == block, scales, 0.0),
        axis=0,
        keepdims=True,
    )
    square = (heads, heads)
    diagonal = lax.broadcasted_iota(jnp.int32, square, 0) == lax.broadcasted_iota(jnp.int32, square, 1)
    column = jnp.sum(jnp.where(diagonal, line, 0.0), axis=1, keepdims=True)
    lane_head = lax.broadcasted_iota(jnp.int32, (heads, rows), 1) % heads
    own_head = lax.broadcasted_iota(jnp.int32, (heads, rows), 0)
    return jnp.sum(jnp.where(lane_head == own_head, column, 0.0), axis=0, keepdims=True)


def kernel(
    n,
    groups,
    heads,
    drafts,
    q_hbm,
    qr_hbm,
    cache_hbm,
    rope_hbm,
    len_ref,
    kq_hbm,
    ks_ref,
    vq_hbm,
    vs_ref,
    w_hbm,
    out_ref,
    q,
    qr,
    cache,
    rope,
    kq,
    vq,
    w,
    cache_t,
    vq_t,
    base,
    lat_all,
    stats,
    out_send,
    out_recv,
    part_send,
    part_recv,
    share_all,
    flat,
    heads_out,
    final,
    in_sem,
    lat_send,
    lat_recv,
    pass_send,
    st_send,
    st_recv,
    o_send,
    o_recv,
    p_send,
    p_recv,
    s_send,
    s_recv,
    f_send,
    f_recv,
):
    me = lax.axis_index("seq")
    group = lax.axis_index("heads")
    rows = q.shape[0]
    cols = lat_all.shape[1]
    width = vq.shape[1]
    positions = cache.shape[0]
    factor = (q.shape[1] + qr.shape[1]) ** (-0.5)

    loads = []
    for i, (src, dst) in enumerate(
        ((kq_hbm, kq), (q_hbm, q), (qr_hbm, qr), (rope_hbm, rope), (cache_hbm, cache), (vq_hbm, vq), (w_hbm, w))
    ):
        copy = pltpu.make_async_copy(src, dst, in_sem.at[i])
        if dst is not w:
            copy.start()
        loads.append(copy)
    kq_load, q_load, qr_load, rope_load, cache_load, vq_load, w_load = loads

    barrier = pltpu.get_barrier_semaphore()

    def greet_seq(j, c):
        pl.semaphore_signal(barrier, inc=1, device_id=(group, lax.rem(me + j, n)), device_id_type=MESH)
        return c

    def greet_heads(j, c):
        pl.semaphore_signal(barrier, inc=1, device_id=(lax.rem(group + j, groups), me), device_id_type=MESH)
        return c

    lax.fori_loop(1, n, greet_seq, 0)
    lax.fori_loop(1, groups, greet_heads, 0)

    def spread(src_of, dst, send, recv):
        def make(j):
            peer = lax.rem(me + j, n)
            return pltpu.make_async_remote_copy(
                src_ref=src_of(peer),
                dst_ref=dst.at[me],
                send_sem=send.at[peer],
                recv_sem=recv.at[me],
                device_id=(group, peer),
                device_id_type=MESH,
            )

        def go(j, c):
            make(j).start()
            return c

        lax.fori_loop(1, n, go, 0)

    def arrive(src_of, dst, send, recv):
        def wait(j, c):
            peer = lax.rem(me + j, n)
            pltpu.make_async_remote_copy(
                src_ref=src_of(peer),
                dst_ref=dst.at[peer],
                send_sem=send.at[peer],
                recv_sem=recv.at[peer],
                device_id=(group, peer),
                device_id_type=MESH,
            ).wait_recv()
            return c

        lax.fori_loop(1, n, wait, 0)

    def drain(src_of, dst, send, recv):
        def wait(j, c):
            peer = lax.rem(me + j, n)
            pltpu.make_async_remote_copy(
                src_ref=src_of(peer),
                dst_ref=dst.at[me],
                send_sem=send.at[peer],
                recv_sem=recv.at[me],
                device_id=(group, peer),
                device_id_type=MESH,
            ).wait_send()
            return c

        lax.fori_loop(1, n, wait, 0)

    block = (me * cols) // QB
    lane_head = lax.broadcasted_iota(jnp.int32, (1, rows), 1) % heads
    key_row = scale_row(ks_ref, block, rows, heads)
    value_row = scale_row(vs_ref, block, rows, heads)

    kq_load.wait()
    q_load.wait()
    every = lax.dot_general(kq[...], q[...], (((1,), (1,)), ((), ())), preferred_element_type=F32)
    every = every.reshape(heads, cols, rows)
    own = lax.broadcasted_iota(jnp.int32, (heads, 1, rows), 0) == lane_head[None]
    piece = jnp.sum(jnp.where(own, every, 0.0), axis=0) * key_row
    lat_all[me] = piece.astype(BF16)

    pl.semaphore_wait(barrier, n - 1 + groups - 1)

    partner = me + 1 - 2 * lax.rem(me, 2)

    def lat_copy(slot, peer, send):
        return pltpu.make_async_remote_copy(
            src_ref=lat_all.at[slot],
            dst_ref=lat_all.at[slot],
            send_sem=send,
            recv_sem=lat_recv.at[slot],
            device_id=(group, peer),
            device_id_type=MESH,
        )

    def like(j):
        return lax.rem(me + 2 * j, n)

    def lat_go(j, c):
        lat_copy(me, like(j), lat_send.at[like(j)]).start()
        return c

    def lat_pass(j, c):
        lat_copy(like(j), partner, pass_send.at[like(j)]).wait_recv()
        lat_copy(like(j), partner, pass_send.at[like(j)]).start()
        return c

    def lat_rest(j, c):
        other = lax.rem(partner + 2 * j, n)
        lat_copy(other, partner, pass_send.at[other]).wait_recv()
        return c

    def lat_drain(j, c):
        lat_copy(me, like(j), lat_send.at[like(j)]).wait_send()
        lat_copy(like(j), partner, pass_send.at[like(j)]).wait_send()
        return c

    lax.fori_loop(1, n // 2, lat_go, 0)
    lat_copy(me, partner, lat_send.at[partner]).start()
    w_load.start()

    qr_load.wait()
    rope_load.wait()
    base[...] = lax.dot_general(
        rope[...].T, qr[...], (((1,), (1,)), ((), ())), preferred_element_type=F32
    )
    lax.fori_loop(1, n // 2, lat_pass, 0)
    cache_load.wait()
    cache_t[...] = cache[...].T
    vq_load.wait()
    vq_t[...] = vq[...].T
    position = me * positions + lax.broadcasted_iota(jnp.int32, (positions, rows), 0)
    horizon = len_ref[0] + lax.broadcasted_iota(jnp.int32, (positions, rows), 1) // heads
    visible = position < horizon

    lax.fori_loop(0, n // 2, lat_rest, 0)
    query_latent = lat_all[...].reshape(n * cols, rows)
    scores = (jnp.dot(cache[...], query_latent, preferred_element_type=F32) + base[...]) * factor
    block_max = jnp.max(jnp.where(visible, scores, neg_large), axis=0, keepdims=True)
    probs = jnp.where(visible, jnp.exp(scores - block_max), 0.0)
    block_sum = jnp.sum(probs, axis=0, keepdims=True)
    stats[me, 0:1, :] = block_max
    stats[me, 1:2, :] = block_sum
    st = (lambda peer: stats.at[me], stats, st_send, st_recv)
    spread(*st)
    block_out = jnp.dot(cache_t[...], probs.astype(BF16), preferred_element_type=F32)
    out_send[...] = block_out.astype(BF16).reshape(n, cols, rows)
    o = (lambda peer: out_send.at[peer], out_recv, o_send, o_recv)
    spread(*o)
    out_recv[me] = out_send[me]

    arrive(*st)
    all_max = stats[:, 0:1, :]
    top = jnp.max(all_max, axis=0, keepdims=True)
    weight = jnp.exp(all_max - top)
    total = jnp.sum(weight * stats[:, 1:2, :], axis=0)
    arrive(*o)
    merged = jnp.sum(out_recv[...].astype(F32) * weight, axis=0) / total
    latent = jnp.where(own, merged[None], 0.0).astype(BF16).reshape(heads * cols, rows)
    partial = jnp.dot(vq_t[...], latent, preferred_element_type=F32) * value_row
    step = width // n
    for d in range(n):
        part_send[d] = partial[d * step : (d + 1) * step].astype(part_send.dtype)
    p = (lambda peer: part_send.at[peer], part_recv, p_send, p_recv)
    spread(*p)
    part_recv[me] = part_send[me]
    arrive(*p)
    share_all[me] = jnp.sum(part_recv[...].astype(F32), axis=0).astype(BF16)
    s = (lambda peer: share_all.at[me], share_all, s_send, s_recv)
    spread(*s)
    arrive(*s)
    head_t = jnp.concatenate([share_all[d].astype(F32) for d in range(n)], axis=0)
    heads_out[...] = head_t.T.reshape(drafts, heads, width)
    for k in range(heads):
        flat[:, k * width : (k + 1) * width] = heads_out[:, k, :].astype(BF16)
    w_load.wait()
    final[group] = lax.dot_general(
        flat[...], w[...], (((1,), (1,)), ((), ())), preferred_element_type=F32
    )

    def pair(j, at):
        peer = lax.rem(group + j, groups)
        return pltpu.make_async_remote_copy(
            src_ref=final.at[group],
            dst_ref=final.at[group if at else peer],
            send_sem=f_send.at[peer],
            recv_sem=f_recv.at[group if at else peer],
            device_id=(peer, me),
            device_id_type=MESH,
        )

    for j in range(1, groups):
        pair(j, True).start()
    for j in range(1, groups):
        pair(j, False).wait_recv()
    out_ref[...] = jnp.sum(final[...], axis=0).astype(BF16)
    for each in (st, o, p, s):
        drain(*each)
    lax.fori_loop(1, n // 2, lat_drain, 0)
    lat_copy(me, partner, lat_send.at[partner]).wait_send()
    for j in range(1, groups):
        pair(j, True).wait_send()


def solution(mesh):
    n = mesh.shape["seq"]
    groups = mesh.shape["heads"]

    def per_device(
        query_nope,
        query_rope,
        latent_cache,
        rope_keys,
        lengths,
        key_quant,
        key_scale,
        value_quant,
        value_scale,
        out_weight,
    ):
        batch, drafts, heads, nope = query_nope.shape
        rows = batch * drafts * heads
        rope = query_rope.shape[-1]
        positions, latent = latent_cache.shape[1:]
        cols = key_quant.shape[1]
        width = value_quant.shape[2]
        model = out_weight.shape[1]
        hbm = pl.BlockSpec(memory_space=pltpu.HBM)
        vmem = pl.BlockSpec(memory_space=pltpu.VMEM)
        smem = pl.BlockSpec(memory_space=pltpu.SMEM)
        dma = pltpu.SemaphoreType.DMA
        result = pl.pallas_call(
            functools.partial(kernel, n, groups, heads, drafts),
            out_shape=jax.ShapeDtypeStruct((drafts, model), BF16),
            in_specs=[hbm, hbm, hbm, hbm, smem, hbm, vmem, hbm, vmem, hbm],
            out_specs=vmem,
            scratch_shapes=[
                pltpu.VMEM((rows, nope), BF16),
                pltpu.VMEM((rows, rope), BF16),
                pltpu.VMEM((positions, latent), BF16),
                pltpu.VMEM((rope, positions), BF16),
                pltpu.VMEM((heads * cols, nope), BF16),
                pltpu.VMEM((heads * cols, width), BF16),
                pltpu.VMEM(out_weight.shape[::-1], BF16),
                pltpu.VMEM((latent, positions), BF16),
                pltpu.VMEM((width, heads * cols), BF16),
                pltpu.VMEM((positions, rows), F32),
                pltpu.VMEM((n, cols, rows), BF16),
                pltpu.VMEM((n, 2, rows), F32),
                pltpu.VMEM((n, cols, rows), BF16),
                pltpu.VMEM((n, cols, rows), BF16),
                pltpu.VMEM((n, width // n, rows), BF16),
                pltpu.VMEM((n, width // n, rows), BF16),
                pltpu.VMEM((n, width // n, rows), BF16),
                pltpu.VMEM((drafts, heads * width), BF16),
                pltpu.VMEM((drafts, heads, width), F32),
                pltpu.VMEM((groups, drafts, model), F32),
                dma((7,)),
            ]
            + [dma((n,))] * 11
            + [dma((groups,))] * 2,
            compiler_params=pltpu.CompilerParams(
                collective_id=0, has_side_effects=True, vmem_limit_bytes=63 * 1024 * 1024
            ),
        )(
            query_nope.reshape(rows, nope),
            query_rope.reshape(rows, rope),
            latent_cache.reshape(positions, latent),
            rope_keys.reshape(rope, positions),
            lengths,
            key_quant.reshape(heads * cols, nope),
            key_scale.T,
            value_quant.reshape(heads * cols, width),
            value_scale.T,
            out_weight.T,
        )
        return result.reshape(batch, drafts, model)

    in_specs = (
        P(None, None, "heads", None),
        P(None, None, "heads", None),
        P(None, "seq", None),
        P(None, None, "seq"),
        P(),
        P("heads", "seq", None),
        P("heads", None),
        P("heads", "seq", None),
        P("heads", None),
        P("heads", "seq"),
    )
    return jax.shard_map(
        per_device, mesh=mesh, in_specs=in_specs, out_specs=P(None, None, "seq"), check_vma=False
    )
```
